32 devices in a mesh: row: 4 (over y, x), col: 8 (over z, core).
Axes of the slice: x: 2, y: 2, z: 4, core: 2. Of those that a mesh axis runs over, the one named last changes fastest.
Arguments:
- strips: int32 [1024, 128, 128], P(('row', 'col')), may hold values from 0 to 1073741824
- grid_pos: int32 [1024], P(('row', 'col')), may hold values from 0 to 1023, as said below
- kernel_spectra: float32 [16, 2, 1024], replicated, may hold values from -6 to 6
- weights: float32 [16], replicated, may hold values from 0.05 to 1
Outputs:
- aerial: float32 [4096, 4096], P('row', 'col')
The draws below stay inside these ranges and needn't reach their ends.
Inputs may be any that keep to these rules, and one draw needn't show every extreme that they name: grid_pos is a permutation of 0 .. 1023; the 32 raster tiles at placement indices d * 32 .. (d + 1) * 32 - 1 lie in 32 different blocks of 1024 x 512 pixels (block (r, c) covers rows r * 1024 onward and columns c * 512 onward), one in each.
All inputs are finite; a program needn't handle non-finite values.
Results may differ from the reference program's by a relative error of at most 0.00005.
Values sent between devices are 32-bit elements; how exact they have to be, the bound alone decides.
A program may use at most 64 MiB of HBM per device.

```python
import math
import jax
import jax.numpy as jnp
from jax import lax

ROWS_DEV = 1024
COLS_DEV = 512
TILE = 128
KF = 32
KERNELS = 16
HALO = 64
WIN = 256
RASTER = 128
STRIPS = 1024
IMG_H = 4096
IMG_W = 4096
N_COL = 8
DEVICES = 32


def draw_grid_pos(key, part):
    key_owner, key_slot = jax.random.split(jax.random.fold_in(key, 7))
    owners = jax.vmap(lambda subkey: jax.random.permutation(subkey, DEVICES))(jax.random.split(key_owner, DEVICES)).astype(jnp.int32)
    slot_table = jax.vmap(lambda subkey: jax.random.permutation(subkey, DEVICES))(jax.random.split(key_slot, DEVICES)).astype(jnp.int32)
    source_ids = jnp.broadcast_to(jnp.arange(DEVICES, dtype=jnp.int32)[:, None], (DEVICES, DEVICES))
    slot_ids = slot_table[owners, source_ids]
    block_rows = ROWS_DEV // RASTER
    block_cols = COLS_DEV // TILE
    strip_row = owners // N_COL * block_rows + slot_ids // block_cols
    strip_col = owners % N_COL * block_cols + slot_ids % block_cols
    return (strip_row * (block_cols * N_COL) + strip_col).reshape(-1).astype(jnp.int32)


def draw_strips(key, part):
    key_col, key_row, key_kind, key_noise = jax.random.split(jax.random.fold_in(key, 11), 4)
    period = 2 * WIN // KF
    half_period = period // 2
    col_phase = jax.random.randint(key_col, (STRIPS, 1, 1), 0, period, dtype=jnp.int32)
    row_phase = jax.random.randint(key_row, (STRIPS, 1, 1), 0, period, dtype=jnp.int32)
    pattern = jax.random.randint(key_kind, (STRIPS, 1, 1), 0, 3, dtype=jnp.int32)
    columns = jnp.arange(TILE, dtype=jnp.int32)[None, None, :]
    rows_here = jnp.arange(RASTER, dtype=jnp.int32)[None, :, None]
    col_on = ((columns + col_phase) % period < half_period).astype(jnp.int32)
    row_on = ((rows_here + row_phase) % period < half_period).astype(jnp.int32)
    covered = jnp.where(pattern == 0, col_on, jnp.where(pattern == 1, row_on, col_on * row_on))
    covered = jnp.broadcast_to(covered, (STRIPS, RASTER, TILE))
    noise = jax.random.randint(key_noise, (STRIPS, RASTER, TILE), 0, 2 ** 28, dtype=jnp.int32)
    first_pixel = (rows_here == 0) & (columns == 0)
    noise = jnp.where(first_pixel, jnp.int32(0), noise)
    return jnp.where(covered == 1, jnp.int32(2 ** 30) - noise, noise).astype(jnp.int32)


def centred(own_key, extent, scale, limit, held_as=jnp.bfloat16):
    return jnp.clip(scale * jax.random.normal(own_key, extent, jnp.float32), -limit, limit).astype(held_as)


def setup_inputs(seed: int = 0) -> dict:
    key_list = jax.random.split(jax.random.key(seed), 5)
    return {
        "strips": draw_strips(jax.random.fold_in(key_list[4], 71), 0),
        "grid_pos": draw_grid_pos(jax.random.fold_in(key_list[4], 71), 0),
        "kernel_spectra": centred(key_list[2], (KERNELS, 2, KF * KF), 1.0, 6.0, jnp.float32),
        "weights": jnp.clip(jnp.exp(jax.random.uniform(key_list[3], (KERNELS,), jnp.float32, math.log(0.05), math.log(1.0))), 0.05, 1.0),
    }


absorber = 0.245
precise = lax.Precision.HIGHEST


def phase_table(length, offset, kept_count, window):
    position = jnp.arange(length, dtype=jnp.int32)[:, None] + offset
    half_kept = kept_count // 2
    frequency = jnp.concatenate([jnp.arange(half_kept, dtype=jnp.int32), jnp.arange(half_kept, dtype=jnp.int32) - half_kept])[None, :]
    phase_steps = (position * frequency) % window
    angles = phase_steps.astype(jnp.float32) * jnp.float32(2.0 * math.pi / window)
    return jnp.cos(angles), jnp.sin(angles)


def aerial_tiles(spec_real, spec_imag, kernel_spectra, weights, tile_size, margin, window):
    kernel_count = kernel_spectra.shape[0]
    kept_count = spec_real.shape[1]
    kern_real = kernel_spectra[:, 0].reshape(kernel_count, kept_count, kept_count)
    kern_imag = kernel_spectra[:, 1].reshape(kernel_count, kept_count, kept_count)
    prod_real = kern_real[:, None] * spec_real[None] - kern_imag[:, None] * spec_imag[None]
    prod_imag = kern_real[:, None] * spec_imag[None] + kern_imag[:, None] * spec_real[None]
    back_cos, back_sin = phase_table(tile_size, margin, kept_count, window)
    half_real = jnp.einsum('pk,nbkl->nbpl', back_cos, prod_real, precision=precise) - jnp.einsum('pk,nbkl->nbpl', back_sin, prod_imag, precision=precise)
    half_imag = jnp.einsum('pk,nbkl->nbpl', back_cos, prod_imag, precision=precise) + jnp.einsum('pk,nbkl->nbpl', back_sin, prod_real, precision=precise)
    field_real = jnp.einsum('nbpl,ql->nbpq', half_real, back_cos, precision=precise) - jnp.einsum('nbpl,ql->nbpq', half_imag, back_sin, precision=precise)
    field_imag = jnp.einsum('nbpl,ql->nbpq', half_real, back_sin, precision=precise) + jnp.einsum('nbpl,ql->nbpq', half_imag, back_cos, precision=precise)
    power = field_real * field_real + field_imag * field_imag
    return jnp.einsum('n,nbpq->bpq', weights, power, precision=precise) / jnp.float32(float(window) ** 4)


def reference(strips, grid_pos, kernel_spectra, weights):
    placed = jnp.zeros_like(strips).at[grid_pos].set(strips)
    raster_cols = IMG_W // TILE
    cover = placed.reshape(IMG_H // RASTER, raster_cols, RASTER, TILE).transpose(0, 2, 1, 3).reshape(IMG_H, IMG_W)
    transmission = 1.0 - (1.0 + absorber) * (cover.astype(jnp.float32) * jnp.float32(2.0 ** -30))
    padded = jnp.pad(transmission, HALO)
    kept_index = jnp.concatenate([jnp.arange(KF // 2, dtype=jnp.int32), jnp.arange(WIN - KF // 2, WIN, dtype=jnp.int32)])

    def one_row(tile_row):
        row_band = lax.dynamic_slice_in_dim(padded, tile_row * TILE, WIN, 0)
        col_blocks = row_band.reshape(WIN, raster_cols + 1, TILE)
        windows = jnp.concatenate([col_blocks[:, :-1], col_blocks[:, 1:]], axis=2).transpose(1, 0, 2)
        spectra = jnp.fft.fft2(windows)[:, kept_index][:, :, kept_index]
        spec_real = jnp.real(spectra).astype(jnp.float32)
        spec_imag = jnp.imag(spectra).astype(jnp.float32)
        intensity = aerial_tiles(spec_real, spec_imag, kernel_spectra, weights, TILE, HALO, WIN)
        return intensity.transpose(1, 0, 2).reshape(TILE, IMG_W)

    rows_out = lax.map(one_row, jnp.arange(IMG_H // TILE, dtype=jnp.int32))
    return rows_out.reshape(IMG_H, IMG_W)
```

```python
import functools

import jax
import jax.numpy as jnp
import numpy as np
from jax import lax
from jax.experimental import pallas as pl
from jax.experimental.pallas import tpu as pltpu
from jax.sharding import PartitionSpec as P

ROWS_DEV = 1024
COLS_DEV = 512
TILE = 128
KF = 32
HALO = TILE // 2
WIN = 2 * TILE
COARSE = 2 * KF
GROUP = 4

absorber = 0.245
bf16 = jnp.bfloat16
f32 = jnp.float32


def halves_of(table):
    high = table.astype(np.float32).astype(bf16)
    low = (table - high.astype(np.float64)).astype(np.float32).astype(bf16)
    return high, low


def frequencies():
    return np.concatenate([np.arange(KF // 2), np.arange(KF // 2) - KF // 2])


def cos_sin(positions):
    angle = 2.0 * np.pi / WIN * ((positions[:, None] * frequencies()[None, :]) % WIN)
    return np.cos(angle), np.sin(angle)


@functools.cache
def tables():
    fwd_cos, fwd_sin = cos_sin(np.arange(WIN))
    col = np.concatenate([np.tile(fwd_cos, (1, GROUP)), np.tile(-fwd_sin, (1, GROUP))], axis=1)
    row = np.block([[fwd_cos.T, fwd_sin.T], [-fwd_sin.T, fwd_cos.T]])
    c, s = cos_sin(np.arange(COARSE) * (WIN // COARSE))
    up = np.block([[c, -s], [s, c]])
    eye = np.eye(GROUP)
    kc, ks = np.kron(eye, c.T), np.kron(eye, s.T)
    across = np.block([[kc, ks], [-ks, kc]])
    shift = (np.arange(TILE) + HALO)[:, None] - (WIN // COARSE) * np.arange(COARSE)[None, :]
    orders = np.arange(1 - KF, KF)
    fine = np.cos(2.0 * np.pi / WIN * ((shift[:, :, None] * orders) % WIN)).sum(-1) / COARSE
    col_hi, col_lo = halves_of(col)
    row_hi, row_lo = halves_of(row)
    up_hi, up_lo = halves_of(up)
    across_hi, across_lo = halves_of(across)
    wide_hi, wide_lo = halves_of(np.tile(fine.T, (GROUP, 1)))
    fine_hi, fine_lo = halves_of(fine)
    return (
        col_hi,
        col_lo,
        row_hi,
        row_lo,
        np.concatenate([up_hi, up_hi, up_lo], axis=1),
        across_hi,
        across_lo,
        wide_hi,
        wide_lo,
        np.concatenate([fine_hi, fine_hi, fine_lo], axis=1),
    )


def mm(a, b):
    return jnp.dot(a, b, preferred_element_type=f32)


def split(x):
    high = x.astype(bf16)
    return high, (x - high.astype(f32)).astype(bf16)


def transmitted(cover):
    return 1.0 - (1.0 + absorber) * (cover.astype(f32) * jnp.float32(2.0 ** (-30)))


def image_kernel(
    place,
    recv,
    top,
    bottom,
    left,
    right,
    kern,
    col_hi,
    col_lo,
    row_hi,
    row_lo,
    up,
    across_hi,
    across_lo,
    wide_hi,
    wide_lo,
    fine,
    out,
    padded,
):
    raster = recv.shape[1] - 8
    block_cols = out.shape[1] // TILE
    block_rows = recv.shape[0] // block_cols
    rows, cols = padded.shape
    step = pl.program_id(0)

    @pl.when(step == 0)
    def _():
        padded[:HALO, HALO : cols - HALO] = top[...]
        padded[rows - HALO :, HALO : cols - HALO] = bottom[...]
        padded[:, :HALO] = left[...]
        padded[:, cols - HALO :] = right[...]

        @pl.loop(0, block_rows)
        def _(i):
            for j in range(block_cols):
                cover = recv[place[i * block_cols + j], :raster, :]
                padded[
                    pl.ds(pl.multiple_of(HALO + i * raster, 8), raster),
                    HALO + j * TILE : HALO + (j + 1) * TILE,
                ] = transmitted(cover)

    first = pl.multiple_of(step * TILE, TILE)
    lanes = GROUP * KF
    groups = kern.shape[2] // lanes
    for j in range(block_cols):
        window = padded[pl.ds(first, WIN), j * TILE : j * TILE + WIN]
        hi, lo = split(window)
        part = mm(hi, col_hi[...]) + mm(lo, col_hi[...]) + mm(hi, col_lo[...])
        part = jnp.concatenate([part[:, :lanes], part[:, lanes:]], axis=0)
        hi, lo = split(part)
        spec = mm(row_hi[...], hi) + mm(row_hi[...], lo) + mm(row_lo[...], hi)
        spec_re = jnp.concatenate([spec[:KF]] * groups, axis=1)
        spec_im = jnp.concatenate([spec[KF:]] * groups, axis=1)
        prod = jnp.concatenate(
            [kern[0] * spec_re - kern[1] * spec_im, kern[0] * spec_im + kern[1] * spec_re], axis=0
        )
        hi, lo = split(prod)
        half = mm(up[...], jnp.concatenate([hi, lo, hi], axis=0))
        half = jnp.concatenate(
            [
                jnp.concatenate(
                    [
                        half[:COARSE, g * lanes : (g + 1) * lanes],
                        half[COARSE:, g * lanes : (g + 1) * lanes],
                    ],
                    axis=1,
                )
                for g in range(groups)
            ],
            axis=0,
        )
        hi, lo = split(half)
        field = mm(hi, across_hi[...]) + mm(lo, across_hi[...]) + mm(hi, across_lo[...])
        wide = field.shape[1] // 2
        power = field[:, :wide] * field[:, :wide] + field[:, wide:] * field[:, wide:]
        power = sum(power[g * COARSE : (g + 1) * COARSE] for g in range(groups))
        hi, lo = split(power)
        power = mm(hi, wide_hi[...]) + mm(lo, wide_hi[...]) + mm(hi, wide_lo[...])
        hi, lo = split(power)
        out[:, j * TILE : (j + 1) * TILE] = mm(fine[...], jnp.concatenate([hi, lo, hi], axis=0))


def image(place, recv, top, bottom, left, right, kern):
    full = lambda shape: pl.BlockSpec(shape, lambda i: (0,) * len(shape))
    whole = [recv, top, bottom, left, right, kern, *(jnp.asarray(t) for t in tables())]
    return pl.pallas_call(
        image_kernel,
        grid=(ROWS_DEV // TILE,),
        in_specs=[pl.BlockSpec(memory_space=pltpu.SMEM)] + [full(a.shape) for a in whole],
        out_specs=pl.BlockSpec((TILE, COLS_DEV), lambda i: (i, 0)),
        out_shape=jax.ShapeDtypeStruct((ROWS_DEV, COLS_DEV), f32),
        scratch_shapes=[pltpu.VMEM((ROWS_DEV + 2 * HALO, COLS_DEV + 2 * HALO), f32)],
        name="image",
    )(place, *whole)


def swap(low_side, high_side, axis):
    count = lax.axis_size(axis)
    forward = [(i, i + 1) for i in range(count - 1)]
    backward = [(i + 1, i) for i in range(count - 1)]
    return lax.ppermute(high_side, axis, forward), lax.ppermute(low_side, axis, backward)


def inverse(keys):
    count = keys.shape[0]
    ids = jnp.arange(count, dtype=jnp.int32)
    return jnp.sum(jnp.where(keys[None, :] == ids[:, None], ids[None, :], 0), axis=1)


def shards(strips, grid_pos, kernel_spectra, weights):
    col_count = lax.axis_size("col")
    count, raster = strips.shape[:2]
    block_rows = ROWS_DEV // raster
    block_cols = COLS_DEV // TILE
    raster_cols = block_cols * col_count
    strip_row = grid_pos // raster_cols
    strip_col = grid_pos % raster_cols
    owners = strip_row // block_rows * col_count + strip_col // block_cols
    slot_ids = strip_row % block_rows * block_cols + strip_col % block_cols
    order = inverse(owners)
    tagged = jnp.concatenate(
        [strips, jnp.broadcast_to(slot_ids[:, None, None], (count, 8, TILE))], axis=1
    )
    received = lax.all_to_all(
        tagged[order], ("row", "col"), split_axis=0, concat_axis=0, tiled=True
    )
    place = inverse(received[:, raster, 0])
    grid = place.reshape(block_rows, block_cols)
    edge_rows = HALO // raster if raster < HALO else 1

    def row_edge(ids, start):
        part = received[ids.reshape(-1), start : start + min(raster, HALO)]
        part = part.reshape(edge_rows, block_cols, -1, TILE).transpose(0, 2, 1, 3)
        return transmitted(part.reshape(HALO, COLS_DEV))

    def col_edge(ids, start):
        return transmitted(received[ids, :raster, start : start + HALO].reshape(ROWS_DEV, HALO))

    top, bottom = swap(
        row_edge(grid[:edge_rows], 0), row_edge(grid[-edge_rows:], max(raster - HALO, 0)), "row"
    )
    left, right = swap(
        jnp.concatenate([top[:, :HALO], col_edge(grid[:, 0], 0), bottom[:, :HALO]], axis=0),
        jnp.concatenate(
            [top[:, -HALO:], col_edge(grid[:, -1], TILE - HALO), bottom[:, -HALO:]], axis=0
        ),
        "col",
    )
    kernels = kernel_spectra.shape[0]
    scale = jnp.sqrt(weights) * jnp.float32(1.0 / WIN**2)
    kern = kernel_spectra.reshape(kernels, 2, KF, KF) * scale[:, None, None, None]
    kern = kern.transpose(1, 2, 0, 3).reshape(2, KF, kernels * KF)
    return image(place, received, top, bottom, left, right, kern)


def solution(mesh):
    return jax.shard_map(
        shards,
        mesh=mesh,
        in_specs=(P(("row", "col"), None, None), P(("row", "col")), P(), P()),
        out_specs=P("row", "col"),
        check_vma=False,
    )
```

```python
import functools
import math

import jax
import jax.numpy as jnp
import numpy as np
from jax import lax
from jax.experimental import pallas as pl
from jax.experimental.pallas import tpu as pltpu
from jax.sharding import PartitionSpec as P

ROWS_DEV = 1024
COLS_DEV = 512
TILE = 128
KF = 32
HALO = TILE // 2
WIN = 2 * TILE
COARSE = 2 * KF
GROUP = 4

absorber = 0.245
bf16 = jnp.bfloat16
f32 = jnp.float32


def halves_of(table):
    high = table.astype(np.float32).astype(bf16)
    low = (table - high.astype(np.float64)).astype(np.float32).astype(bf16)
    return high, low


def frequencies():
    return np.concatenate([np.arange(KF // 2), np.arange(KF // 2) - KF // 2])


def cos_sin(positions):
    angle = 2.0 * np.pi / WIN * ((positions[:, None] * frequencies()[None, :]) % WIN)
    return np.cos(angle), np.sin(angle)


def sums_of(length):
    if length < HALO:
        return np.eye(length)
    x = np.arange(length) - (length - 1) / 2
    angle = 2.0 * np.pi / WIN * np.arange(KF // 2 + 1)[:, None] * x[None, :]
    return np.concatenate([np.cos(angle), np.sin(angle[1:])])


def phases_of(length):
    k = frequencies()
    first = np.arange(WIN // length) * length
    if length < HALO:
        place = first[:, None] + np.arange(length)[None, :]
        return np.exp(-2j * np.pi / WIN * (k[:, None, None] * place[None] % WIN))
    centre = first + (length - 1) / 2
    turn = np.exp(-2j * np.pi / WIN * k[:, None] * centre[None, :])
    pick = np.zeros((KF, KF + 1), complex)
    for i, f in enumerate(k):
        pick[i, abs(f)] = 1.0
        if f != 0:
            pick[i, KF // 2 + abs(f)] = -1j * np.sign(f)
    return turn[:, :, None] * pick[:, None, :]


def sent_rows(length):
    return -(-(sums_of(length).shape[0] + 3) // 8) * 8


@functools.cache
def pack_tables(raster):
    length = min(raster, HALO)
    parts = raster // length
    row = sums_of(length)
    count, rows = row.shape[0], sent_rows(length)
    across = np.kron(np.eye(2), sums_of(HALO)).reshape(2, KF + 1, TILE)
    main = across[:, :KF].reshape(2 * KF, TILE).T
    main = np.concatenate([main] * parts + [np.zeros((TILE, TILE - parts * 2 * KF))], axis=1)
    extra = np.zeros((rows, TILE))
    extra[count : count + 2] = across[:, KF]
    down = np.zeros((rows, raster))
    down[:count] = np.tile(row, (1, parts))
    turned = np.zeros((raster, TILE))
    for p in range(parts):
        turned[p * length : (p + 1) * length, p * 2 * KF : p * 2 * KF + count] = row.T
    return (*halves_of(main), *halves_of(extra), *halves_of(down), *halves_of(turned))


@functools.cache
def tables(raster):
    length = min(raster, HALO)
    parts = raster // length
    count, rows = sums_of(length).shape[0], sent_rows(length)
    phase = phases_of(HALO)
    lanes = GROUP * KF
    main = np.zeros((3, TILE, parts, 2, GROUP, KF))
    extra = np.zeros((3, 8, 2, GROUP, KF))
    for segment, (tile, half) in enumerate([(0, 1), (1, 0), (1, 1), (2, 0)]):
        for ri, value in enumerate([phase[:, segment].real, phase[:, segment].imag]):
            for p in range(parts):
                at = p * 2 * KF + half * KF
                main[tile, at : at + KF, p, ri] = value.T[:KF, None, :]
            extra[tile, count % 8 + half, ri] = value.T[KF, None, :]
    main = main.reshape(3 * TILE, parts * 2 * lanes)
    extra = extra.reshape(24, 2 * lanes)
    down = np.zeros((KF, WIN // length, rows), complex)
    down[:, :, :count] = phases_of(length)
    down = down.reshape(KF, -1)
    row = np.block([[down.real, -down.imag], [down.imag, down.real]])
    c, s = cos_sin(np.arange(COARSE) * (WIN // COARSE))
    up = np.block([[c, -s], [s, c]])
    eye = np.eye(GROUP)
    kc, ks = np.kron(eye, c.T), np.kron(eye, s.T)
    across = np.block([[kc, ks], [-ks, kc]])
    shift = (np.arange(TILE) + HALO)[:, None] - (WIN // COARSE) * np.arange(COARSE)[None, :]
    orders = np.arange(1 - KF, KF)
    fine = np.cos(2.0 * np.pi / WIN * ((shift[:, :, None] * orders) % WIN)).sum(-1) / COARSE
    up_hi, up_lo = halves_of(up)
    fine_hi, fine_lo = halves_of(fine)
    return (
        *halves_of(main),
        *halves_of(extra),
        *halves_of(row),
        np.concatenate([up_hi, up_hi, up_lo], axis=1),
        *halves_of(across),
        *halves_of(np.tile(fine.T, (GROUP, 1))),
        np.concatenate([fine_hi, fine_hi, fine_lo], axis=1),
    )


def mm(a, b):
    return jnp.dot(a, b, preferred_element_type=f32)


def split(x):
    high = x.astype(bf16)
    return high, (x - high.astype(f32)).astype(bf16)


def dot3(a, b, dims=((1,), (0,))):
    dot = lambda x, y: lax.dot_general(x, y, (dims, ((), ())), preferred_element_type=f32)
    return dot(a[0], b[0]) + dot(a[1], b[0]) + dot(a[0], b[1])


def transmitted(cover):
    return 1.0 - (1.0 + absorber) * (cover.astype(f32) * jnp.float32(2.0 ** (-30)))


def pack_kernel(
    order,
    slots,
    strips,
    main_hi,
    main_lo,
    extra_hi,
    extra_lo,
    down_hi,
    down_lo,
    turned_hi,
    turned_lo,
    out,
):
    count, rows, _ = out.shape
    raster = strips.shape[1]
    length = min(raster, HALO)
    sums = sums_of(length).shape[0]
    batch = math.gcd(count, 8)
    row_part = lax.broadcasted_iota(jnp.int32, (raster, TILE), 0) // length
    lane_part = lax.broadcasted_iota(jnp.int32, (raster, TILE), 1) // (2 * KF)
    keep = row_part == lane_part
    slot_row = lax.broadcasted_iota(jnp.int32, (rows, TILE), 0) == sums + 2
    main, extra = (main_hi[...], main_lo[...]), (extra_hi[...], extra_lo[...])
    down, turned = (down_hi[...], down_lo[...]), (turned_hi[...], turned_lo[...])

    @pl.loop(0, count // batch)
    def _(i):
        for j in range(batch):
            at = i * batch + j
            pixels = split(transmitted(strips[order[at]]))
            wide = jnp.where(keep, dot3(pixels, main), 0.0)
            sent = dot3(down, split(wide))
            turn = dot3(extra, pixels, ((1,), (1,)))
            sent = sent + dot3(split(turn), turned)
            out[at] = jnp.where(slot_row, slots[at], sent)


def pack(order, slots, strips):
    count, raster, _ = strips.shape
    consts = [jnp.asarray(t) for t in pack_tables(raster)]
    smem, vmem = pl.BlockSpec(memory_space=pltpu.SMEM), pl.BlockSpec(memory_space=pltpu.VMEM)
    return pl.pallas_call(
        pack_kernel,
        in_specs=[smem, smem] + [vmem] * (1 + len(consts)),
        out_specs=vmem,
        out_shape=jax.ShapeDtypeStruct((count, sent_rows(min(raster, HALO)), TILE), f32),
        name="pack",
    )(order, slots, strips, *consts)


def image_kernel(
    raster,
    place,
    recv,
    top,
    bottom,
    left,
    right,
    kern,
    main_hi,
    main_lo,
    extra_hi,
    extra_lo,
    row_hi,
    row_lo,
    up,
    across_hi,
    across_lo,
    wide_hi,
    wide_lo,
    fine,
    out,
    sums,
    partial,
):
    length = min(raster, HALO)
    parts = raster // length
    kept = sums_of(length).shape[0]
    rows = recv.shape[1]
    block_cols = out.shape[1] // TILE
    block_rows = recv.shape[0] // block_cols
    edge = top.shape[0] // block_cols
    ext_rows = block_rows + 2 * edge
    step = pl.program_id(0)
    lanes = GROUP * KF

    @pl.when(step == 0)
    def _():
        @pl.loop(0, block_rows)
        def _(i):
            for j in range(block_cols):
                at = pl.ds(pl.multiple_of((i + edge) * rows, 8), rows)
                sums[at, (j + 1) * TILE : (j + 2) * TILE] = recv[place[i * block_cols + j]]

        for i in range(edge):
            for j in range(block_cols):
                at = slice((j + 1) * TILE, (j + 2) * TILE)
                sums[i * rows : (i + 1) * rows, at] = top[i * block_cols + j]
                k = ext_rows - edge + i
                sums[k * rows : (k + 1) * rows, at] = bottom[i * block_cols + j]

        main, extra = (main_hi[...], main_lo[...]), (extra_hi[...], extra_lo[...])

        @pl.loop(0, ext_rows)
        def _(i):
            at = pl.ds(pl.multiple_of(i * rows, 8), rows)
            sums[at, :TILE] = left[i]
            sums[at, (block_cols + 1) * TILE :] = right[i]

        @pl.loop(0, ext_rows)
        def _(i):
            at = pl.ds(pl.multiple_of(i * rows, 8), rows)
            for j in range(block_cols):
                tiles = sums[at, j * TILE : (j + 3) * TILE]
                got = dot3(split(tiles), main)
                first = kept // 8 * 8
                ends = jnp.concatenate(
                    [tiles[first : first + 8, t * TILE : (t + 1) * TILE] for t in range(3)], axis=0
                )
                more = dot3(split(ends), extra, ((0,), (0,)))
                for p in range(parts):
                    to = pl.multiple_of((i * parts + p) * rows, 8)
                    partial[j, pl.ds(to, rows), :] = (
                        got[:, p * 2 * lanes : (p + 1) * 2 * lanes]
                        + more[p * 2 * KF : p * 2 * KF + rows]
                    )

    first = pl.multiple_of(
        (step * (TILE // length) + edge * parts - HALO // length) * rows, 8
    )
    groups = kern.shape[2] // lanes
    for j in range(block_cols):
        part = partial[j, pl.ds(first, WIN // length * rows), :]
        part = jnp.concatenate([part[:, :lanes], part[:, lanes:]], axis=0)
        hi, lo = split(part)
        spec = mm(row_hi[...], hi) + mm(row_hi[...], lo) + mm(row_lo[...], hi)
        spec_re = jnp.concatenate([spec[:KF]] * groups, axis=1)
        spec_im = jnp.concatenate([spec[KF:]] * groups, axis=1)
        prod = jnp.concatenate(
            [kern[0] * spec_re - kern[1] * spec_im, kern[0] * spec_im + kern[1] * spec_re], axis=0
        )
        hi, lo = split(prod)
        half = mm(up[...], jnp.concatenate([hi, lo, hi], axis=0))
        half = jnp.concatenate(
            [
                jnp.concatenate(
                    [
                        half[:COARSE, g * lanes : (g + 1) * lanes],
                        half[COARSE:, g * lanes : (g + 1) * lanes],
                    ],
                    axis=1,
                )
                for g in range(groups)
            ],
            axis=0,
        )
        hi, lo = split(half)
        field = mm(hi, across_hi[...]) + mm(lo, across_hi[...]) + mm(hi, across_lo[...])
        wide = field.shape[1] // 2
        power = field[:, :wide] * field[:, :wide] + field[:, wide:] * field[:, wide:]
        power = sum(power[g * COARSE : (g + 1) * COARSE] for g in range(groups))
        hi, lo = split(power)
        power = mm(hi, wide_hi[...]) + mm(lo, wide_hi[...]) + mm(hi, wide_lo[...])
        hi, lo = split(power)
        out[:, j * TILE : (j + 1) * TILE] = mm(fine[...], jnp.concatenate([hi, lo, hi], axis=0))


def image(raster, place, recv, top, bottom, left, right, kern):
    full = lambda shape: pl.BlockSpec(shape, lambda i: (0,) * len(shape))
    consts = [jnp.asarray(t) for t in tables(raster)]
    whole = [recv, top, bottom, left, right, kern, *consts]
    block_cols = COLS_DEV // TILE
    ext_rows, rows, _ = left.shape
    parts = max(raster // HALO, 1)
    return pl.pallas_call(
        functools.partial(image_kernel, raster),
        grid=(ROWS_DEV // TILE,),
        in_specs=[pl.BlockSpec(memory_space=pltpu.SMEM)] + [full(a.shape) for a in whole],
        out_specs=pl.BlockSpec((TILE, COLS_DEV), lambda i: (i, 0)),
        out_shape=jax.ShapeDtypeStruct((ROWS_DEV, COLS_DEV), f32),
        scratch_shapes=[
            pltpu.VMEM((ext_rows * rows, (block_cols + 2) * TILE), f32),
            pltpu.VMEM((block_cols, ext_rows * parts * rows, 2 * GROUP * KF), f32),
        ],
        name="image",
    )(place, *whole)


def swap(low_side, high_side, axis):
    count = lax.axis_size(axis)
    forward = [(i, i + 1) for i in range(count - 1)]
    backward = [(i + 1, i) for i in range(count - 1)]
    return lax.ppermute(high_side, axis, forward), lax.ppermute(low_side, axis, backward)


def inverse(keys):
    count = keys.shape[0]
    ids = jnp.arange(count, dtype=jnp.int32)
    return jnp.sum(jnp.where(keys[None, :] == ids[:, None], ids[None, :], 0), axis=1)


def shards(strips, grid_pos, kernel_spectra, weights):
    col_count = lax.axis_size("col")
    count, raster = strips.shape[:2]
    block_rows = ROWS_DEV // raster
    block_cols = COLS_DEV // TILE
    raster_cols = block_cols * col_count
    strip_row = grid_pos // raster_cols
    strip_col = grid_pos % raster_cols
    owners = strip_row // block_rows * col_count + strip_col // block_cols
    slot_ids = strip_row % block_rows * block_cols + strip_col % block_cols
    order = inverse(owners)
    sent = pack(order, slot_ids.astype(f32)[order], strips)
    received = lax.all_to_all(sent, ("row", "col"), split_axis=0, concat_axis=0, tiled=True)
    slot_row = sums_of(min(raster, HALO)).shape[0] + 2
    place = inverse(received[:, slot_row, 0].astype(jnp.int32))
    grid = place.reshape(block_rows, block_cols)
    edge = max(HALO // raster, 1)
    top, bottom = swap(
        received[grid[:edge].reshape(-1)], received[grid[-edge:].reshape(-1)], "row"
    )
    left, right = swap(
        jnp.concatenate([top[::block_cols], received[grid[:, 0]], bottom[::block_cols]]),
        jnp.concatenate(
            [
                top[block_cols - 1 :: block_cols],
                received[grid[:, -1]],
                bottom[block_cols - 1 :: block_cols],
            ]
        ),
        "col",
    )
    kernels = kernel_spectra.shape[0]
    scale = jnp.sqrt(weights) * jnp.float32(1.0 / WIN**2)
    kern = kernel_spectra.reshape(kernels, 2, KF, KF) * scale[:, None, None, None]
    kern = kern.transpose(1, 2, 0, 3).reshape(2, KF, kernels * KF)
    return image(raster, place, received, top, bottom, left, right, kern)


def solution(mesh):
    return jax.shard_map(
        shards,
        mesh=mesh,
        in_specs=(P(("row", "col"), None, None), P(("row", "col")), P(), P()),
        out_specs=P("row", "col"),
        check_vma=False,
    )
```

```python
import functools
import math

import jax
import jax.numpy as jnp
import numpy as np
from jax import lax
from jax.experimental import pallas as pl
from jax.experimental.pallas import tpu as pltpu
from jax.sharding import PartitionSpec as P

ROWS_DEV = 1024
COLS_DEV = 512
TILE = 128
KF = 32
HALO = TILE // 2
WIN = 2 * TILE
COARSE = 2 * KF
GROUP = 4

absorber = 0.245
bf16 = jnp.bfloat16
f32 = jnp.float32


def halves_of(table):
    high = table.astype(np.float32).astype(bf16)
    low = (table - high.astype(np.float64)).astype(np.float32).astype(bf16)
    return high, low


def frequencies():
    return np.concatenate([np.arange(KF // 2), np.arange(KF // 2) - KF // 2])


def cos_sin(positions):
    angle = 2.0 * np.pi / WIN * ((positions[:, None] * frequencies()[None, :]) % WIN)
    return np.cos(angle), np.sin(angle)


def sums_of(length):
    if length < HALO:
        return np.eye(length)
    x = np.arange(length) - (length - 1) / 2
    angle = 2.0 * np.pi / WIN * np.arange(KF // 2 + 1)[:, None] * x[None, :]
    return np.concatenate([np.cos(angle), np.sin(angle[1:])])


def phases_of(length):
    k = frequencies()
    first = np.arange(WIN // length) * length
    if length < HALO:
        place = first[:, None] + np.arange(length)[None, :]
        return np.exp(-2j * np.pi / WIN * (k[:, None, None] * place[None] % WIN))
    centre = first + (length - 1) / 2
    turn = np.exp(-2j * np.pi / WIN * k[:, None] * centre[None, :])
    pick = np.zeros((KF, KF + 1), complex)
    for i, f in enumerate(k):
        pick[i, abs(f)] = 1.0
        if f != 0:
            pick[i, KF // 2 + abs(f)] = -1j * np.sign(f)
    return turn[:, :, None] * pick[:, None, :]


def sent_rows(length):
    return -(-(sums_of(length).shape[0] + 3) // 8) * 8


@functools.cache
def pack_tables(raster):
    length = min(raster, HALO)
    parts = raster // length
    row = sums_of(length)
    count, rows = row.shape[0], sent_rows(length)
    across = np.kron(np.eye(2), sums_of(HALO)).reshape(2, KF + 1, TILE)
    main = across[:, :KF].reshape(2 * KF, TILE).T
    main = np.concatenate([main] * parts + [np.zeros((TILE, TILE - parts * 2 * KF))], axis=1)
    extra = np.zeros((8, TILE))
    extra[count - rows + 8 : count - rows + 10] = across[:, KF]
    down = np.zeros((rows, raster))
    down[:count] = np.tile(row, (1, parts))
    turned = np.zeros((raster, TILE))
    for p in range(parts):
        turned[p * length : (p + 1) * length, p * 2 * KF : p * 2 * KF + count] = row.T
    return (*halves_of(main), *halves_of(extra), *halves_of(down), *halves_of(turned))


@functools.cache
def tables(raster):
    length = min(raster, HALO)
    parts = raster // length
    count, rows = sums_of(length).shape[0], sent_rows(length)
    phase = phases_of(HALO)
    lanes = GROUP * KF
    main = np.zeros((3, TILE, parts, 2, GROUP, KF))
    extra = np.zeros((3, 8, 2, GROUP, KF))
    for segment, (tile, half) in enumerate([(0, 1), (1, 0), (1, 1), (2, 0)]):
        for ri, value in enumerate([phase[:, segment].real, phase[:, segment].imag]):
            for p in range(parts):
                at = p * 2 * KF + half * KF
                main[tile, at : at + KF, p, ri] = value.T[:KF, None, :]
            extra[tile, count % 8 + half, ri] = value.T[KF, None, :]
    main = main.reshape(3 * TILE, parts * 2 * lanes)
    extra = extra.reshape(24, 2 * lanes)
    down = np.zeros((KF, WIN // length, rows), complex)
    down[:, :, :count] = phases_of(length)
    down = down.reshape(KF, -1)
    row = np.block([[down.real, -down.imag], [down.imag, down.real]])
    c, s = cos_sin(np.arange(COARSE) * (WIN // COARSE))
    up = np.block([[c, -s], [s, c]])
    eye = np.eye(GROUP)
    kc, ks = np.kron(eye, c.T), np.kron(eye, s.T)
    across = np.block([[kc, ks], [-ks, kc]])
    shift = (np.arange(TILE) + HALO)[:, None] - (WIN // COARSE) * np.arange(COARSE)[None, :]
    orders = np.arange(1 - KF, KF)
    fine = np.cos(2.0 * np.pi / WIN * ((shift[:, :, None] * orders) % WIN)).sum(-1) / COARSE
    up_hi, up_lo = halves_of(up)
    fine_hi, fine_lo = halves_of(fine)
    return (
        *halves_of(main),
        *halves_of(extra),
        *halves_of(row),
        np.concatenate([up_hi, up_hi, up_lo], axis=1),
        *halves_of(across),
        *halves_of(np.tile(fine.T, (GROUP, 1))),
        np.concatenate([fine_hi, fine_hi, fine_lo], axis=1),
    )


def mm(a, b):
    return jnp.dot(a, b, preferred_element_type=f32)


def split(x):
    high = x.astype(bf16)
    return high, (x - high.astype(f32)).astype(bf16)


def dot3(a, b, dims=((1,), (0,))):
    dot = lambda x, y: lax.dot_general(x, y, (dims, ((), ())), preferred_element_type=f32)
    return dot(a[0], b[0]) + dot(a[1], b[0]) + dot(a[0], b[1])


def transmitted(cover):
    return 1.0 - (1.0 + absorber) * (cover.astype(f32) * jnp.float32(2.0 ** (-30)))


def pack_kernel(
    order,
    slots,
    strips,
    main_hi,
    main_lo,
    extra_hi,
    extra_lo,
    down_hi,
    down_lo,
    turned_hi,
    turned_lo,
    out,
):
    count, rows, _ = out.shape
    raster = strips.shape[1]
    length = min(raster, HALO)
    sums = sums_of(length).shape[0]
    batch = math.gcd(count, 8)
    row_part = lax.broadcasted_iota(jnp.int32, (raster, TILE), 0) // length
    lane_part = lax.broadcasted_iota(jnp.int32, (raster, TILE), 1) // (2 * KF)
    keep = row_part == lane_part
    last = rows - 8
    slot_row = lax.broadcasted_iota(jnp.int32, (8, TILE), 0) == sums + 2 - last
    main, extra = (main_hi[...], main_lo[...]), (extra_hi[...], extra_lo[...])
    down, turned = (down_hi[...], down_lo[...]), (turned_hi[...], turned_lo[...])

    @pl.loop(0, count // batch)
    def _(i):
        pixels = jnp.concatenate([strips[order[i * batch + j]] for j in range(batch)], axis=0)
        pixels = split(transmitted(pixels))
        wide = dot3(pixels, main)
        wide = jnp.concatenate(
            [jnp.where(keep, wide[j * raster : (j + 1) * raster], 0.0) for j in range(batch)],
            axis=1,
        )
        sent = dot3(down, split(wide))
        turn = dot3(extra, pixels, ((1,), (1,)))
        turn = jnp.concatenate(
            [turn[:, j * raster : (j + 1) * raster] for j in range(batch)], axis=0
        )
        more = dot3(split(turn), turned)
        for j in range(batch):
            at = i * batch + j
            out[at, :last] = sent[:last, j * TILE : (j + 1) * TILE]
            out[at, last:] = jnp.where(
                slot_row,
                slots[at],
                sent[last:, j * TILE : (j + 1) * TILE] + more[j * 8 : (j + 1) * 8],
            )


def pack(order, slots, strips):
    count, raster, _ = strips.shape
    consts = [jnp.asarray(t) for t in pack_tables(raster)]
    smem, vmem = pl.BlockSpec(memory_space=pltpu.SMEM), pl.BlockSpec(memory_space=pltpu.VMEM)
    return pl.pallas_call(
        pack_kernel,
        in_specs=[smem, smem] + [vmem] * (1 + len(consts)),
        out_specs=vmem,
        out_shape=jax.ShapeDtypeStruct((count, sent_rows(min(raster, HALO)), TILE), f32),
        name="pack",
    )(order, slots, strips, *consts)


def image_kernel(
    raster,
    place,
    recv,
    top,
    bottom,
    left,
    right,
    kern,
    main_hi,
    main_lo,
    extra_hi,
    extra_lo,
    row_hi,
    row_lo,
    up,
    across_hi,
    across_lo,
    wide_hi,
    wide_lo,
    fine,
    out,
    sums,
    partial,
):
    length = min(raster, HALO)
    parts = raster // length
    kept = sums_of(length).shape[0]
    rows = recv.shape[1]
    block_cols = out.shape[1] // TILE
    block_rows = recv.shape[0] // block_cols
    edge = top.shape[0] // block_cols
    ext_rows = block_rows + 2 * edge
    step = pl.program_id(0)
    lanes = GROUP * KF

    @pl.when(step == 0)
    def _():
        @pl.loop(0, block_rows)
        def _(i):
            for j in range(block_cols):
                at = pl.ds(pl.multiple_of((i + edge) * rows, 8), rows)
                sums[at, (j + 1) * TILE : (j + 2) * TILE] = recv[place[i * block_cols + j]]

        for i in range(edge):
            for j in range(block_cols):
                at = slice((j + 1) * TILE, (j + 2) * TILE)
                sums[i * rows : (i + 1) * rows, at] = top[i * block_cols + j]
                k = ext_rows - edge + i
                sums[k * rows : (k + 1) * rows, at] = bottom[i * block_cols + j]

        main, extra = (main_hi[...], main_lo[...]), (extra_hi[...], extra_lo[...])

        @pl.loop(0, ext_rows)
        def _(i):
            at = pl.ds(pl.multiple_of(i * rows, 8), rows)
            sums[at, :TILE] = left[i]
            sums[at, (block_cols + 1) * TILE :] = right[i]

        first = kept // 8 * 8
        for j in range(block_cols):
            got = dot3(split(sums[:, j * TILE : (j + 3) * TILE]), main)
            ends = [
                [
                    sums[i * rows + first : i * rows + first + 8, t * TILE : (t + 1) * TILE]
                    for i in range(ext_rows)
                ]
                for t in range(j, j + 3)
            ]
            ends = jnp.concatenate([jnp.concatenate(e, axis=1) for e in ends], axis=0)
            more = dot3(split(ends), extra, ((0,), (0,)))
            for i in range(ext_rows):
                for p in range(parts):
                    to, at = (i * parts + p) * rows, i * TILE + p * 2 * KF
                    partial[j, to : to + rows, :] = (
                        got[i * rows : (i + 1) * rows, p * 2 * lanes : (p + 1) * 2 * lanes]
                        + more[at : at + rows]
                    )

    first = pl.multiple_of(
        (step * (TILE // length) + edge * parts - HALO // length) * rows, 8
    )
    groups = kern.shape[2] // lanes
    span = kern.shape[2]
    part = [partial[j, pl.ds(first, WIN // length * rows), :] for j in range(block_cols)]
    part = jnp.concatenate(
        [jnp.concatenate([y[:, ri * lanes : (ri + 1) * lanes] for y in part], axis=1) for ri in (0, 1)],
        axis=0,
    )
    spec = dot3((row_hi[...], row_lo[...]), split(part))
    prods = []
    for j in range(block_cols):
        spec_re = jnp.concatenate([spec[:KF, j * lanes : (j + 1) * lanes]] * groups, axis=1)
        spec_im = jnp.concatenate([spec[KF:, j * lanes : (j + 1) * lanes]] * groups, axis=1)
        prod = jnp.concatenate(
            [kern[0] * spec_re - kern[1] * spec_im, kern[0] * spec_im + kern[1] * spec_re], axis=0
        )
        hi, lo = split(prod)
        prods.append(jnp.concatenate([hi, lo, hi], axis=0))
    half = mm(up[...], jnp.concatenate(prods, axis=1))
    half = jnp.concatenate(
        [
            jnp.concatenate(
                [half[:COARSE, at : at + lanes], half[COARSE:, at : at + lanes]], axis=1
            )
            for at in range(0, block_cols * span, lanes)
        ],
        axis=0,
    )
    field = dot3(split(half), (across_hi[...], across_lo[...]))
    wide = field.shape[1] // 2
    power = field[:, :wide] * field[:, :wide] + field[:, wide:] * field[:, wide:]
    power = [
        sum(power[(j * groups + g) * COARSE : (j * groups + g + 1) * COARSE] for g in range(groups))
        for j in range(block_cols)
    ]
    power = dot3(split(jnp.concatenate(power, axis=0)), (wide_hi[...], wide_lo[...]))
    power = jnp.concatenate(
        [power[j * COARSE : (j + 1) * COARSE] for j in range(block_cols)], axis=1
    )
    hi, lo = split(power)
    out[...] = mm(fine[...], jnp.concatenate([hi, lo, hi], axis=0))


def image(raster, place, recv, top, bottom, left, right, kern):
    full = lambda shape: pl.BlockSpec(shape, lambda i: (0,) * len(shape))
    consts = [jnp.asarray(t) for t in tables(raster)]
    whole = [recv, top, bottom, left, right, kern, *consts]
    block_cols = COLS_DEV // TILE
    ext_rows, rows, _ = left.shape
    parts = max(raster // HALO, 1)
    return pl.pallas_call(
        functools.partial(image_kernel, raster),
        grid=(ROWS_DEV // TILE,),
        in_specs=[pl.BlockSpec(memory_space=pltpu.SMEM)] + [full(a.shape) for a in whole],
        out_specs=pl.BlockSpec((TILE, COLS_DEV), lambda i: (i, 0)),
        out_shape=jax.ShapeDtypeStruct((ROWS_DEV, COLS_DEV), f32),
        scratch_shapes=[
            pltpu.VMEM((ext_rows * rows, (block_cols + 2) * TILE), f32),
            pltpu.VMEM((block_cols, ext_rows * parts * rows, 2 * GROUP * KF), f32),
        ],
        name="image",
    )(place, *whole)


def swap(low_side, high_side, axis):
    count = lax.axis_size(axis)
    forward = [(i, i + 1) for i in range(count - 1)]
    backward = [(i + 1, i) for i in range(count - 1)]
    return lax.ppermute(high_side, axis, forward), lax.ppermute(low_side, axis, backward)


def inverse(keys):
    count = keys.shape[0]
    ids = jnp.arange(count, dtype=jnp.int32)
    return jnp.sum(jnp.where(keys[None, :] == ids[:, None], ids[None, :], 0), axis=1)


def shards(strips, grid_pos, kernel_spectra, weights):
    col_count = lax.axis_size("col")
    count, raster = strips.shape[:2]
    block_rows = ROWS_DEV // raster
    block_cols = COLS_DEV // TILE
    raster_cols = block_cols * col_count
    strip_row = grid_pos // raster_cols
    strip_col = grid_pos % raster_cols
    owners = strip_row // block_rows * col_count + strip_col // block_cols
    slot_ids = strip_row % block_rows * block_cols + strip_col % block_cols
    order = inverse(owners)
    sent = pack(order, slot_ids.astype(f32)[order], strips)
    received = lax.all_to_all(sent, ("row", "col"), split_axis=0, concat_axis=0, tiled=True)
    slot_row = sums_of(min(raster, HALO)).shape[0] + 2
    place = inverse(received[:, slot_row, 0].astype(jnp.int32))
    grid = place.reshape(block_rows, block_cols)
    edge = max(HALO // raster, 1)
    top, bottom = swap(
        received[grid[:edge].reshape(-1)], received[grid[-edge:].reshape(-1)], "row"
    )
    left, right = swap(
        jnp.concatenate([top[::block_cols], received[grid[:, 0]], bottom[::block_cols]]),
        jnp.concatenate(
            [
                top[block_cols - 1 :: block_cols],
                received[grid[:, -1]],
                bottom[block_cols - 1 :: block_cols],
            ]
        ),
        "col",
    )
    kernels = kernel_spectra.shape[0]
    scale = jnp.sqrt(weights) * jnp.float32(1.0 / WIN**2)
    kern = kernel_spectra.reshape(kernels, 2, KF, KF) * scale[:, None, None, None]
    kern = kern.transpose(1, 2, 0, 3).reshape(2, KF, kernels * KF)
    return image(raster, place, received, top, bottom, left, right, kern)


def solution(mesh):
    return jax.shard_map(
        shards,
        mesh=mesh,
        in_specs=(P(("row", "col"), None, None), P(("row", "col")), P(), P()),
        out_specs=P("row", "col"),
        check_vma=False,
    )
```

```python
import functools
import math

import jax
import jax.numpy as jnp
import numpy as np
from jax import lax
from jax.experimental import pallas as pl
from jax.experimental.pallas import tpu as pltpu
from jax.sharding import PartitionSpec as P

ROWS_DEV = 1024
COLS_DEV = 512
TILE = 128
KF = 32
HALO = TILE // 2
WIN = 2 * TILE
COARSE = 2 * KF
GROUP = 4

absorber = 0.245
bf16 = jnp.bfloat16
f32 = jnp.float32


def halves_of(table):
    high = table.astype(np.float32).astype(bf16)
    low = (table - high.astype(np.float64)).astype(np.float32).astype(bf16)
    return high, low


def frequencies():
    return np.concatenate([np.arange(KF // 2), np.arange(KF // 2) - KF // 2])


def cos_sin(positions):
    angle = 2.0 * np.pi / WIN * ((positions[:, None] * frequencies()[None, :]) % WIN)
    return np.cos(angle), np.sin(angle)


def sums_of(length):
    if length < HALO:
        return np.eye(length)
    x = np.arange(length) - (length - 1) / 2
    angle = 2.0 * np.pi / WIN * np.arange(KF // 2 + 1)[:, None] * x[None, :]
    return np.concatenate([np.cos(angle), np.sin(angle[1:])])


def phases_of(length):
    k = frequencies()
    first = np.arange(WIN // length) * length
    if length < HALO:
        place = first[:, None] + np.arange(length)[None, :]
        return np.exp(-2j * np.pi / WIN * (k[:, None, None] * place[None] % WIN))
    centre = first + (length - 1) / 2
    turn = np.exp(-2j * np.pi / WIN * k[:, None] * centre[None, :])
    pick = np.zeros((KF, KF + 1), complex)
    for i, f in enumerate(k):
        pick[i, abs(f)] = 1.0
        if f != 0:
            pick[i, KF // 2 + abs(f)] = -1j * np.sign(f)
    return turn[:, :, None] * pick[:, None, :]


def sent_rows(length):
    return -(-(sums_of(length).shape[0] + 3) // 8) * 8


@functools.cache
def pack_tables(raster):
    length = min(raster, HALO)
    parts = raster // length
    row = sums_of(length)
    count, rows = row.shape[0], sent_rows(length)
    across = np.kron(np.eye(2), sums_of(HALO)).reshape(2, KF + 1, TILE)
    main = across[:, :KF].reshape(2 * KF, TILE).T
    main = np.concatenate([main] * parts + [np.zeros((TILE, TILE - parts * 2 * KF))], axis=1)
    extra = np.zeros((8, TILE))
    extra[count - rows + 8 : count - rows + 10] = across[:, KF]
    down = np.zeros((rows, raster))
    down[:count] = np.tile(row, (1, parts))
    turned = np.zeros((raster, TILE))
    for p in range(parts):
        turned[p * length : (p + 1) * length, p * 2 * KF : p * 2 * KF + count] = row.T
    return (*halves_of(main), *halves_of(extra), *halves_of(down), *halves_of(turned))


@functools.cache
def tables(raster):
    length = min(raster, HALO)
    parts = raster // length
    count, rows = sums_of(length).shape[0], sent_rows(length)
    phase = phases_of(HALO)
    lanes = GROUP * KF
    main = np.zeros((3, TILE, parts, 2, GROUP, KF))
    extra = np.zeros((3, 8, 2, GROUP, KF))
    for segment, (tile, half) in enumerate([(0, 1), (1, 0), (1, 1), (2, 0)]):
        for ri, value in enumerate([phase[:, segment].real, phase[:, segment].imag]):
            for p in range(parts):
                at = p * 2 * KF + half * KF
                main[tile, at : at + KF, p, ri] = value.T[:KF, None, :]
            extra[tile, count % 8 + half, ri] = value.T[KF, None, :]
    main = main.reshape(3 * TILE, parts * 2 * lanes)
    extra = extra.reshape(24, 2 * lanes)
    down = np.zeros((KF, WIN // length, rows), complex)
    down[:, :, :count] = phases_of(length)
    down = down.reshape(KF, -1)
    row = np.block([[down.real, -down.imag], [down.imag, down.real]])
    c, s = cos_sin(np.arange(COARSE) * (WIN // COARSE))
    up = np.block([[c, -s], [s, c]])
    eye = np.eye(GROUP)
    kc, ks = np.kron(eye, c.T), np.kron(eye, s.T)
    across = np.block([[kc, ks], [-ks, kc]])
    shift = (np.arange(TILE) + HALO)[:, None] - (WIN // COARSE) * np.arange(COARSE)[None, :]
    orders = np.arange(1 - KF, KF)
    fine = np.cos(2.0 * np.pi / WIN * ((shift[:, :, None] * orders) % WIN)).sum(-1) / COARSE
    up_hi, up_lo = halves_of(up)
    fine_hi, fine_lo = halves_of(fine)
    return (
        *halves_of(main),
        *halves_of(extra),
        *halves_of(row),
        np.concatenate([up_hi, up_hi, up_lo], axis=1),
        *halves_of(across),
        *halves_of(np.tile(fine.T, (GROUP, 1))),
        np.concatenate([fine_hi, fine_hi, fine_lo], axis=1),
    )


def mm(a, b):
    return jnp.dot(a, b, preferred_element_type=f32)


def split(x):
    high = x.astype(bf16)
    return high, (x - high.astype(f32)).astype(bf16)


def dot3(a, b, dims=((1,), (0,))):
    dot = lambda x, y: lax.dot_general(x, y, (dims, ((), ())), preferred_element_type=f32)
    return dot(a[0], b[0]) + dot(a[1], b[0]) + dot(a[0], b[1])


def transmitted(cover):
    return 1.0 - (1.0 + absorber) * (cover.astype(f32) * jnp.float32(2.0 ** (-30)))


def pack_kernel(
    owners,
    slots,
    strips,
    main_hi,
    main_lo,
    extra_hi,
    extra_lo,
    down_hi,
    down_lo,
    turned_hi,
    turned_lo,
    out,
):
    rows = out.shape[1]
    batch, raster, _ = strips.shape
    length = min(raster, HALO)
    sums = sums_of(length).shape[0]
    row_part = lax.broadcasted_iota(jnp.int32, (raster, TILE), 0) // length
    lane_part = lax.broadcasted_iota(jnp.int32, (raster, TILE), 1) // (2 * KF)
    keep = row_part == lane_part
    last = rows - 8
    slot_row = lax.broadcasted_iota(jnp.int32, (8, TILE), 0) == sums + 2 - last
    main, extra = (main_hi[...], main_lo[...]), (extra_hi[...], extra_lo[...])
    down, turned = (down_hi[...], down_lo[...]), (turned_hi[...], turned_lo[...])

    pixels = strips[...].reshape(batch * raster, TILE)
    pixels = split(transmitted(pixels))
    wide = dot3(pixels, main)
    wide = jnp.concatenate(
        [jnp.where(keep, wide[j * raster : (j + 1) * raster], 0.0) for j in range(batch)],
        axis=1,
    )
    sent = dot3(down, split(wide))
    turn = dot3(extra, pixels, ((1,), (1,)))
    turn = jnp.concatenate(
        [turn[:, j * raster : (j + 1) * raster] for j in range(batch)], axis=0
    )
    more = dot3(split(turn), turned)
    for j in range(batch):
        s = pl.program_id(0) * batch + j
        at = owners[s]
        out[at, :last] = sent[:last, j * TILE : (j + 1) * TILE]
        out[at, last:] = jnp.where(
            slot_row,
            slots[s],
            sent[last:, j * TILE : (j + 1) * TILE] + more[j * 8 : (j + 1) * 8],
        )


def pack(owners, slots, strips):
    count, raster, _ = strips.shape
    rows = sent_rows(min(raster, HALO))
    batch = math.gcd(count, 8)
    consts = [jnp.asarray(t) for t in pack_tables(raster)]
    smem = pl.BlockSpec(memory_space=pltpu.SMEM)
    return pl.pallas_call(
        pack_kernel,
        grid=(count // batch,),
        in_specs=[smem, smem, pl.BlockSpec((batch, raster, TILE), lambda i: (i, 0, 0))]
        + [pl.BlockSpec(t.shape, lambda i: (0, 0)) for t in consts],
        out_specs=pl.BlockSpec((count, rows, TILE), lambda i: (0, 0, 0)),
        out_shape=jax.ShapeDtypeStruct((count, rows, TILE), f32),
        name="pack",
    )(owners, slots, strips, *consts)


def image_kernel(
    raster,
    place,
    recv,
    top,
    bottom,
    left,
    right,
    kern,
    main_hi,
    main_lo,
    extra_hi,
    extra_lo,
    row_hi,
    row_lo,
    up,
    across_hi,
    across_lo,
    wide_hi,
    wide_lo,
    fine,
    out,
    sums,
    partial,
):
    length = min(raster, HALO)
    parts = raster // length
    kept = sums_of(length).shape[0]
    rows = recv.shape[1]
    block_cols = out.shape[1] // TILE
    block_rows = recv.shape[0] // block_cols
    edge = top.shape[0] // block_cols
    ext_rows = block_rows + 2 * edge
    step = pl.program_id(0)
    lanes = GROUP * KF

    @pl.when(step == 0)
    def _():
        @pl.loop(0, block_rows)
        def _(i):
            for j in range(block_cols):
                at = pl.ds(pl.multiple_of((i + edge) * rows, 8), rows)
                sums[at, (j + 1) * TILE : (j + 2) * TILE] = recv[place[i * block_cols + j]]

        for i in range(edge):
            for j in range(block_cols):
                at = slice((j + 1) * TILE, (j + 2) * TILE)
                sums[i * rows : (i + 1) * rows, at] = top[i * block_cols + j]
                k = ext_rows - edge + i
                sums[k * rows : (k + 1) * rows, at] = bottom[i * block_cols + j]

        main, extra = (main_hi[...], main_lo[...]), (extra_hi[...], extra_lo[...])

        @pl.loop(0, ext_rows)
        def _(i):
            at = pl.ds(pl.multiple_of(i * rows, 8), rows)
            sums[at, :TILE] = left[i]
            sums[at, (block_cols + 1) * TILE :] = right[i]

        first = kept // 8 * 8
        for j in range(block_cols):
            got = dot3(split(sums[:, j * TILE : (j + 3) * TILE]), main)
            ends = [
                [
                    sums[i * rows + first : i * rows + first + 8, t * TILE : (t + 1) * TILE]
                    for i in range(ext_rows)
                ]
                for t in range(j, j + 3)
            ]
            ends = jnp.concatenate([jnp.concatenate(e, axis=1) for e in ends], axis=0)
            more = dot3(split(ends), extra, ((0,), (0,)))
            for i in range(ext_rows):
                for p in range(parts):
                    to, at = (i * parts + p) * rows, i * TILE + p * 2 * KF
                    partial[j, to : to + rows, :] = (
                        got[i * rows : (i + 1) * rows, p * 2 * lanes : (p + 1) * 2 * lanes]
                        + more[at : at + rows]
                    )

    first = pl.multiple_of(
        (step * (TILE // length) + edge * parts - HALO // length) * rows, 8
    )
    groups = kern.shape[2] // lanes
    span = kern.shape[2]
    part = [partial[j, pl.ds(first, WIN // length * rows), :] for j in range(block_cols)]
    part = jnp.concatenate(
        [jnp.concatenate([y[:, ri * lanes : (ri + 1) * lanes] for y in part], axis=1) for ri in (0, 1)],
        axis=0,
    )
    spec = dot3((row_hi[...], row_lo[...]), split(part))
    prods = []
    for j in range(block_cols):
        spec_re = jnp.concatenate([spec[:KF, j * lanes : (j + 1) * lanes]] * groups, axis=1)
        spec_im = jnp.concatenate([spec[KF:, j * lanes : (j + 1) * lanes]] * groups, axis=1)
        prod = jnp.concatenate(
            [kern[0] * spec_re - kern[1] * spec_im, kern[0] * spec_im + kern[1] * spec_re], axis=0
        )
        hi, lo = split(prod)
        prods.append(jnp.concatenate([hi, lo, hi], axis=0))
    half = mm(up[...], jnp.concatenate(prods, axis=1))
    half = jnp.concatenate(
        [
            jnp.concatenate(
                [half[:COARSE, at : at + lanes], half[COARSE:, at : at + lanes]], axis=1
            )
            for at in range(0, block_cols * span, lanes)
        ],
        axis=0,
    )
    field = dot3(split(half), (across_hi[...], across_lo[...]))
    wide = field.shape[1] // 2
    power = field[:, :wide] * field[:, :wide] + field[:, wide:] * field[:, wide:]
    power = [
        sum(power[(j * groups + g) * COARSE : (j * groups + g + 1) * COARSE] for g in range(groups))
        for j in range(block_cols)
    ]
    power = dot3(split(jnp.concatenate(power, axis=0)), (wide_hi[...], wide_lo[...]))
    power = jnp.concatenate(
        [power[j * COARSE : (j + 1) * COARSE] for j in range(block_cols)], axis=1
    )
    hi, lo = split(power)
    out[...] = mm(fine[...], jnp.concatenate([hi, lo, hi], axis=0))


def image(raster, place, recv, top, bottom, left, right, kern):
    full = lambda shape: pl.BlockSpec(shape, lambda i: (0,) * len(shape))
    consts = [jnp.asarray(t) for t in tables(raster)]
    whole = [recv, top, bottom, left, right, kern, *consts]
    block_cols = COLS_DEV // TILE
    ext_rows, rows, _ = left.shape
    parts = max(raster // HALO, 1)
    return pl.pallas_call(
        functools.partial(image_kernel, raster),
        grid=(ROWS_DEV // TILE,),
        in_specs=[pl.BlockSpec(memory_space=pltpu.SMEM)] + [full(a.shape) for a in whole],
        out_specs=pl.BlockSpec((TILE, COLS_DEV), lambda i: (i, 0)),
        out_shape=jax.ShapeDtypeStruct((ROWS_DEV, COLS_DEV), f32),
        scratch_shapes=[
            pltpu.VMEM((ext_rows * rows, (block_cols + 2) * TILE), f32),
            pltpu.VMEM((block_cols, ext_rows * parts * rows, 2 * GROUP * KF), f32),
        ],
        name="image",
    )(place, *whole)


def swap(low_side, high_side, axis):
    count = lax.axis_size(axis)
    forward = [(i, i + 1) for i in range(count - 1)]
    backward = [(i + 1, i) for i in range(count - 1)]
    return lax.ppermute(high_side, axis, forward), lax.ppermute(low_side, axis, backward)


def inverse(keys):
    count = keys.shape[0]
    ids = jnp.arange(count, dtype=jnp.int32)
    return jnp.sum(jnp.where(keys[None, :] == ids[:, None], ids[None, :], 0), axis=1)


def shards(strips, grid_pos, kernel_spectra, weights):
    col_count = lax.axis_size("col")
    count, raster = strips.shape[:2]
    block_rows = ROWS_DEV // raster
    block_cols = COLS_DEV // TILE
    raster_cols = block_cols * col_count
    strip_row = grid_pos // raster_cols
    strip_col = grid_pos % raster_cols
    owners = strip_row // block_rows * col_count + strip_col // block_cols
    slot_ids = strip_row % block_rows * block_cols + strip_col % block_cols
    sent = pack(owners, slot_ids.astype(f32), strips)
    received = lax.all_to_all(sent, ("row", "col"), split_axis=0, concat_axis=0, tiled=True)
    slot_row = sums_of(min(raster, HALO)).shape[0] + 2
    place = inverse(received[:, slot_row, 0].astype(jnp.int32))
    grid = place.reshape(block_rows, block_cols)
    edge = max(HALO // raster, 1)
    top, bottom = swap(
        received[grid[:edge].reshape(-1)], received[grid[-edge:].reshape(-1)], "row"
    )
    left, right = swap(
        jnp.concatenate([top[::block_cols], received[grid[:, 0]], bottom[::block_cols]]),
        jnp.concatenate(
            [
                top[block_cols - 1 :: block_cols],
                received[grid[:, -1]],
                bottom[block_cols - 1 :: block_cols],
            ]
        ),
        "col",
    )
    kernels = kernel_spectra.shape[0]
    scale = jnp.sqrt(weights) * jnp.float32(1.0 / WIN**2)
    kern = kernel_spectra.reshape(kernels, 2, KF, KF) * scale[:, None, None, None]
    kern = kern.transpose(1, 2, 0, 3).reshape(2, KF, kernels * KF)
    return image(raster, place, received, top, bottom, left, right, kern)


def solution(mesh):
    return jax.shard_map(
        shards,
        mesh=mesh,
        in_specs=(P(("row", "col"), None, None), P(("row", "col")), P(), P()),
        out_specs=P("row", "col"),
        check_vma=False,
    )
```
